128 devices in a mesh: lat: 64 (over z, y, x), fld: 2 (over core).
Axes of the slice: x: 4, y: 4, z: 4, core: 2. Of those that a mesh axis runs over, the one named last changes fastest.
Arguments:
- grid: bfloat16 [2, 4, 69, 640, 1408], P('fld', None, None, 'lat'), may hold values from -6 to 6
- cycle_ids: int32 [640], replicated, may hold values from 0 to 639, each once
- cycle_len: int32 [640], replicated, may hold values from 20 to 1296, as said below
- wave_ids: int32 [320], replicated, may hold values from 0 to 319, each once
- legendre: bfloat16 [320, 320, 640], P('lat'), may hold values from -0.25 to 0.25
- target: float32 [2, 4, 69, 2, 320, 320], P('fld', None, None, None, 'lat'), may hold values from -18 to 18
- step_w: float32 [2], P('fld'), may hold values from 0.5 to 2
- chan_w: float32 [69], replicated, may hold values from 0.2 to 2
Outputs:
- coeffs: float32 [2, 4, 69, 2, 320, 320], P('fld', None, None, None, 'lat')
- loss: float32 [], replicated
- field_grad: bfloat16 [2, 4, 69, 640, 1408], P('fld', None, None, 'lat')
The draws below stay inside these ranges and needn't reach their ends.
Inputs may be any that keep to these rules, and one draw needn't show every extreme that they name: `cycle_len`: every length 20 + 4 j with j from 0 to 319 occurs exactly twice.
All inputs are finite; a program needn't handle non-finite values.
Results may differ from the reference program's by a relative error of at most 0.0065.
Values may be sent and summed in bfloat16 or wider, within the bound.
A program may use at most 256 MiB of HBM per device.

```python
import math
import jax
import jax.numpy as jnp
from jax import lax

R = 640
MW = 320
CH = 69
BATCH = 4
STEPS = 2
SEG = 1408


def draw_cycle_len(key, part):
    order = jax.random.permutation(jax.random.fold_in(key, 11), R).astype(jnp.int32)
    return (20 + 4 * (order // 2)).astype(jnp.int32)


def draw_target(key, part):
    shape = (STEPS, BATCH, CH, 2, MW, MW)
    slot_index = jnp.arange(MW, dtype=jnp.float32) / (MW - 1)
    values = jnp.clip(jax.random.normal(jax.random.fold_in(key, 22), shape, jnp.float32), -6.0, 6.0)
    slot_scale = 0.5 + 2.5 * slot_index
    return (values * slot_scale[:, None]).astype(jnp.float32)


def steps_of(rng, extent, cuts, least, top_value):
    factor_of, own = 1.0, jax.random.fold_in(rng, 6)
    for axis_at, parts in cuts:
        draws = jnp.exp(jax.random.uniform(jax.random.fold_in(own, axis_at), (parts,), jnp.float32, least / len(cuts), top_value / len(cuts)))
        factor_of = factor_of * jnp.repeat(draws, extent[axis_at] // parts).reshape([-1 if axis == axis_at else 1 for axis in range(len(extent))])
    return factor_of


def scatter_about(rng, dims, spread, bound, shards=(), kind=jnp.bfloat16):
    gain = steps_of(rng, dims, shards, -0.22, 0.18) if shards else 1.0
    result = jax.random.normal(rng, dims, jnp.float32) * spread * gain
    return jnp.minimum(jnp.maximum(result, -bound), bound).astype(kind)


def setup_inputs(seed: int = 0) -> dict:
    keys = jax.random.split(jax.random.key(seed), 9)
    return {
        "grid": scatter_about(keys[0], (STEPS, BATCH, CH, R, SEG), 1.0, 6.0, ((0, 2), (3, 64))),
        "cycle_ids": jax.random.permutation(keys[1], R).astype(jnp.int32),
        "cycle_len": draw_cycle_len(jax.random.fold_in(keys[8], 71), 0),
        "wave_ids": jax.random.permutation(keys[3], MW).astype(jnp.int32),
        "legendre": scatter_about(keys[4], (MW, MW, R), R ** -0.5, 0.25, ((0, 64),)),
        "target": draw_target(jax.random.fold_in(keys[8], 71), 0),
        "step_w": jnp.clip(jnp.exp(math.log(2.0) - 1.3862944 * jax.random.uniform(keys[6], (STEPS,), jnp.float32) ** steps_of(keys[6], (STEPS,), ((0, 2),), -0.2, 0.2)), 0.5, 2.0),
        "chan_w": jnp.clip(jnp.exp(jax.random.uniform(keys[7], (CH,), jnp.float32, math.log(0.2), math.log(2.0))), 0.2, 2.0),
    }


def cycle_table(length, wave_order, segment):
    slot_index = jnp.arange(segment, dtype=jnp.int32)
    phase_int = slot_index[:, None] * wave_order[None, :] % length
    angles = 2.0 * math.pi / length.astype(jnp.float32) * phase_int.astype(jnp.float32)
    inside = (slot_index[:, None] < length) & (2 * wave_order[None, :] < length)
    row_scale = jnp.where(inside, lax.rsqrt(length.astype(jnp.float32)), jnp.float32(0.0))
    paired = jnp.stack([jnp.cos(angles) * row_scale, -jnp.sin(angles) * row_scale], axis=2)
    return paired.reshape(segment, 2 * wave_order.shape[0]).astype(jnp.bfloat16)

def reference(grid, cycle_ids, cycle_len, wave_ids, legendre, target, step_w, chan_w):
    step_count, batch_size, chan_count, cycle_count, segment = grid.shape
    wave_count = wave_ids.shape[0]
    col_count = step_count * batch_size * chan_count
    highest = lax.Precision.HIGHEST

    def forward_cycle(cycle_slot):
        length = cycle_len[cycle_ids[cycle_slot]]
        dft_table = cycle_table(length, wave_ids, segment).astype(jnp.float32)
        grid_rows = lax.dynamic_index_in_dim(grid, cycle_slot, 3, keepdims=False)
        grid_rows = grid_rows.reshape(col_count, segment).astype(jnp.float32)
        return jnp.dot(grid_rows, dft_table, precision=highest).astype(jnp.bfloat16)
    fourier = lax.map(forward_cycle, jnp.arange(cycle_count, dtype=jnp.int32))
    fourier = fourier.reshape(cycle_count, col_count, wave_count, 2)
    basis_all = jnp.take(legendre, cycle_ids, axis=2)
    degree = jnp.arange(wave_count, dtype=jnp.int32)
    weight_cols = jnp.broadcast_to(step_w[:, None, None] * chan_w[None, None, :], (step_count, batch_size, chan_count)).reshape(col_count)

    def per_slot(wave_slot):
        basis = lax.dynamic_index_in_dim(basis_all, wave_slot, 0, keepdims=False).astype(jnp.float32)
        slot_fourier = lax.dynamic_index_in_dim(fourier, wave_slot, 2, keepdims=False)
        slot_fourier = slot_fourier.astype(jnp.float32).reshape(cycle_count, col_count * 2)
        coeffs = jnp.dot(basis, slot_fourier, precision=highest).reshape(wave_count, col_count, 2)
        wave_num = wave_ids[wave_slot]
        kept_mask = (degree >= wave_num).astype(jnp.float32)[:, None, None]
        coeffs = coeffs * kept_mask
        target_slot = lax.dynamic_index_in_dim(target, wave_slot, 4, keepdims=False)
        target_slot = jnp.transpose(target_slot.reshape(col_count, 2, wave_count), (2, 0, 1))
        factor = jnp.where(wave_num == 0, 1.0, 2.0).astype(jnp.float32)
        weight = (factor * weight_cols)[None, :, None]
        misfit = (coeffs - target_slot) * kept_mask
        partial_value = jnp.sum(weight * misfit * misfit)
        grad_coeff = (2.0 * weight * misfit).astype(jnp.bfloat16)
        back_rows = jnp.dot(basis.T, grad_coeff.astype(jnp.float32).reshape(wave_count, col_count * 2), precision=highest).astype(jnp.bfloat16)
        return (jnp.transpose(coeffs, (1, 2, 0)), partial_value, back_rows.reshape(cycle_count, col_count, 2))
    coeff_all, partials, back_all = lax.map(per_slot, jnp.arange(wave_count, dtype=jnp.int32))
    coeff_all = coeff_all.reshape(wave_count, step_count, batch_size, chan_count, 2, wave_count)
    coeffs = jnp.moveaxis(coeff_all, 0, 4)

    def adjoint_cycle(cycle_slot):
        length = cycle_len[cycle_ids[cycle_slot]]
        dft_table = cycle_table(length, wave_ids, segment).astype(jnp.float32)
        slot_back = lax.dynamic_index_in_dim(back_all, cycle_slot, 1, keepdims=False)
        slot_back = jnp.transpose(slot_back, (1, 0, 2)).reshape(col_count, 2 * wave_count)
        return jnp.dot(slot_back.astype(jnp.float32), dft_table.T, precision=highest).astype(jnp.bfloat16)
    field_rows = lax.map(adjoint_cycle, jnp.arange(cycle_count, dtype=jnp.int32))
    field_rows = field_rows.reshape(cycle_count, step_count, batch_size, chan_count, segment)
    field_grad = jnp.moveaxis(field_rows, 0, 3)
    term_count = step_count * batch_size * chan_count * wave_count * (wave_count + 1) // 2
    loss = jnp.sum(partials) / jnp.float32(term_count)
    return (coeffs, loss, field_grad)
```

```python
import functools
import math

import jax
import jax.numpy as jnp
import numpy as np
from jax import lax
from jax.experimental import pallas as pl
from jax.experimental.pallas import tpu as pltpu
from jax.sharding import Mesh
from jax.sharding import PartitionSpec as P

STEPS = 2
LAT = ("lat_0", "lat_1", "lat_2")
LAT_FLD = ("lat_0", "lat_1", "lat_2", "fld")
N_LAT = 64
ROWS = 232
TILE_ROWS = 104
LO = 32
HI = 44
F32 = jnp.float32
BF16 = jnp.bfloat16


def _fit():
    node = np.cos(np.pi * (np.arange(64) + 0.5) / 64)
    w = 0.125 * (node + 1.0)
    u = np.sqrt(w)
    cos_fit = np.polynomial.chebyshev.Chebyshev.fit(w, np.cos(2 * np.pi * u), 8, domain=[0, 0.25])
    sin_fit = np.polynomial.chebyshev.Chebyshev.fit(
        w, np.sin(2 * np.pi * u) / u, 8, domain=[0, 0.25]
    )
    as_power = lambda fit: [float(v) for v in fit.convert(kind=np.polynomial.Polynomial).coef]
    return as_power(cos_fit), as_power(sin_fit)


COS_POLY, SIN_POLY = _fit()


def turn_cos_sin(turn):
    turn = turn - jnp.round(turn)
    w = turn * turn
    c = jnp.full_like(w, COS_POLY[-1])
    s = jnp.full_like(w, SIN_POLY[-1])
    for cc, sc in zip(COS_POLY[-2::-1], SIN_POLY[-2::-1]):
        c = c * w + cc
        s = s * w + sc
    return c, s * turn


def turn_of(points, waves, length, inverse):
    product = points * waves
    whole = jnp.round(product * inverse)
    return (product - whole * length) * inverse


def make_table(length, inverse, scale, wave_ref, quarter_ref, cos_hi, sin_hi, cos_lo, sin_lo, table_ref):
    waves = wave_ref[...]
    cols = waves.shape[1]
    points = lax.broadcasted_iota(jnp.int32, (48, cols), 0).astype(F32) * float(LO)
    c, s = turn_cos_sin(turn_of(points, waves, length, inverse))
    gain = jnp.where(2.0 * waves < length, scale, 0.0)
    cos_hi[...] = c * gain
    sin_hi[...] = s * gain
    points = lax.broadcasted_iota(jnp.int32, (LO, cols), 0).astype(F32)
    c, s = turn_cos_sin(turn_of(points, waves, length, inverse) + quarter_ref[...])
    cos_lo[...] = c
    sin_lo[...] = s

    def step(i, carry):
        a = cos_hi[pl.ds(i, 1), :]
        b = sin_hi[pl.ds(i, 1), :]
        rows = pl.multiple_of(i * LO, LO)
        table_ref[0, pl.ds(rows, LO), :] = (a * cos_lo[...] - b * sin_lo[...]).astype(BF16)
        return carry

    return step


def forward_kernel(
    len_ref, inv_ref, scale_ref, grid_ref, wave_ref, quarter_ref, out_ref, table_ref,
    cos_hi, sin_hi, cos_lo, sin_lo, lhs, acc, packed,
):
    p = pl.program_id(0)
    length = len_ref[p]
    flength = length.astype(F32)
    step = make_table(
        flength, inv_ref[p], scale_ref[p], wave_ref, quarter_ref,
        cos_hi, sin_hi, cos_lo, sin_lo, table_ref,
    )
    tiles = (length + 255) // 256
    lax.fori_loop(0, jnp.minimum(tiles * (256 // LO), HI), step, 0)
    seg = lhs.shape[1]
    inside = (lax.broadcasted_iota(jnp.int32, (1, seg), 1) < length).astype(F32).astype(BF16)
    for c in range(69):
        lhs[4 * c : 4 * c + 4, :] = grid_ref[c, 0] * inside
    for n in range(1, 7):
        depth = min(256 * n, seg)

        @pl.when(tiles == n)
        def _():
            acc[...] = jnp.dot(
                lhs[:, :depth], table_ref[0, :depth, :], preferred_element_type=F32
            )

    for s in range(5):
        for tile in range(2):
            block = acc[tile * 128 : tile * 128 + 128, s * 128 : s * 128 + 128].T
            for part in range(2):
                start = tile * TILE_ROWS + (part * 5 + s) * 10
                packed[pl.ds(start + p, N_LAT, ROWS), :] = block[part * 64 : part * 64 + 64]
    rest = [acc[256:280, s * 128 : s * 128 + 128] for s in range(5)]
    rest = jnp.concatenate(rest + [jnp.zeros((8, 128), F32)], axis=0).T
    for part in range(2):
        start = 2 * TILE_ROWS + part * 10
        packed[pl.ds(start + p, N_LAT, ROWS), :] = rest[part * 64 : part * 64 + 64]

    @pl.when(p == pl.num_programs(0) - 1)
    def _():
        def move(i, carry):
            rows = pl.multiple_of(i * ROWS, 8)
            out_ref[i] = packed[pl.ds(rows, ROWS), :].astype(BF16)
            return carry

        lax.fori_loop(0, N_LAT, move, 0)


def order_kernel(ids_ref, leg_ref, out_ref, out_t_ref, pick):
    @pl.when(pl.program_id(0) == 0)
    def _():
        q = lax.broadcasted_iota(jnp.int32, (640, 640), 0)
        pick[...] = (q == ids_ref[...]).astype(F32).astype(BF16)

    ordered = jnp.dot(leg_ref[0], pick[...], preferred_element_type=F32)
    out_ref[0] = ordered.astype(BF16)
    out_t_ref[0] = ordered.T.astype(BF16)


def owner_kernel(
    wave_ref, recv_ref, leg_ref, leg_t_ref, target_ref, weight_ref,
    send_ref, coeff_ref, loss_ref, packed, rhs, grad, spread, rest_back,
):
    s = pl.program_id(0)

    @pl.when(s == 0)
    def _():
        def move(i, carry):
            rows = pl.multiple_of(i * ROWS, 8)
            packed[pl.ds(rows, ROWS), :] = recv_ref[i].astype(F32)
            return carry

        lax.fori_loop(0, N_LAT, move, 0)
        for part in range(2):
            for p in range(10):
                start = 2 * TILE_ROWS + part * 10 + p
                rhs[p * 64 : p * 64 + 64, 512 + part * 128 : 640 + part * 128] = packed[
                    pl.ds(start, N_LAT, ROWS), :
                ].astype(BF16)
        loss_ref[...] = jnp.zeros_like(loss_ref)
        rest_back[...] = jnp.zeros_like(rest_back)

    for part in range(2):
        for tile in range(2):
            for p in range(10):
                start = tile * TILE_ROWS + part * 50 + p
                lanes = part * 256 + tile * 128
                rhs[p * 64 : p * 64 + 64, lanes : lanes + 128] = packed[
                    pl.ds(start + s * 10, N_LAT, ROWS), :
                ].astype(BF16)
    wave = wave_ref[s]
    kept_t = lax.broadcasted_iota(jnp.int32, (320, 128), 0) >= wave
    kept = lax.broadcasted_iota(jnp.int32, (1, 320), 1) >= wave
    factor = jnp.where(wave == 0, 1.0, 2.0).astype(F32)
    group = pl.ds(pl.multiple_of(s * 24, 8), 24)
    total = jnp.zeros((8, 320), F32)
    for tile in range(3):
        for part in range(2):
            lanes = part * 256 + tile * 128 if tile < 2 else 512 + part * 128
            block = jnp.dot(leg_ref[0], rhs[:, lanes : lanes + 128], preferred_element_type=F32)
            block = jnp.where(kept_t, block, 0.0).T
            if tile == 2:
                spread[...] = block
                block = spread[group, :]
            rows = block.shape[0]
            base = tile * 128
            coeff_ref[0, part, base : base + rows, :] = block
            weight = factor * weight_ref[base : base + rows, :]
            misfit = jnp.where(kept, block - target_ref[0, part, base : base + rows, :], 0.0)
            pulled = weight * misfit
            square = pulled * misfit
            if tile == 2:
                square = jnp.where(
                    lax.broadcasted_iota(jnp.int32, (24, 1), 0) < 20, square, 0.0
                )
            total = total + square.reshape(rows // 8, 8, 320).sum(axis=0)
            if tile == 2:
                spread[...] = jnp.zeros_like(spread)
                spread[group, :] = 2.0 * pulled
                grad[part, 256:384, :] = spread[...].astype(BF16)
            else:
                grad[part, base : base + rows, :] = (2.0 * pulled).astype(BF16)
    loss_ref[...] += total
    for part in range(2):
        back = lax.dot_general(
            leg_t_ref[0], grad[part], (((1,), (1,)), ((), ())), preferred_element_type=F32
        )
        for tile in range(2):
            for p in range(10):
                start = tile * TILE_ROWS + part * 50 + p
                packed[pl.ds(start + s * 10, N_LAT, ROWS), :] = back[
                    p * 64 : p * 64 + 64, tile * 128 : tile * 128 + 128
                ]
        rest_back[part] += back[:, 256:384]

    @pl.when(s == pl.num_programs(0) - 1)
    def _():
        for part in range(2):
            for p in range(10):
                start = 2 * TILE_ROWS + part * 10 + p
                packed[pl.ds(start, N_LAT, ROWS), :] = rest_back[part, p * 64 : p * 64 + 64, :]

        def move(i, carry):
            rows = pl.multiple_of(i * ROWS, 8)
            send_ref[i] = packed[pl.ds(rows, ROWS), :].astype(BF16)
            return carry

        lax.fori_loop(0, N_LAT, move, 0)


def adjoint_kernel(len_ref, recv_ref, table_ref, out_ref, packed, lhs, field):
    p = pl.program_id(0)
    length = len_ref[p]

    @pl.when(p == 0)
    def _():
        def move(i, carry):
            rows = pl.multiple_of(i * ROWS, 8)
            packed[pl.ds(rows, ROWS), :] = recv_ref[i].astype(F32)
            return carry

        lax.fori_loop(0, N_LAT, move, 0)

    for s in range(5):
        for tile in range(2):
            halves = [
                packed[pl.ds(tile * TILE_ROWS + (part * 5 + s) * 10 + p, N_LAT, ROWS), :]
                for part in range(2)
            ]
            lhs[tile * 128 : tile * 128 + 128, s * 128 : s * 128 + 128] = (
                jnp.concatenate(halves, axis=0).T.astype(BF16)
            )
    halves = [
        packed[pl.ds(2 * TILE_ROWS + part * 10 + p, N_LAT, ROWS), :] for part in range(2)
    ]
    rest = jnp.concatenate(halves, axis=0).T
    for s in range(5):
        lhs[256:280, s * 128 : s * 128 + 128] = rest[s * 24 : s * 24 + 24].astype(BF16)
    seg = field.shape[1]
    for n in range(6):
        first, last = 256 * n, min(256 * n + 256, seg)

        @pl.when(first < length)
        def _():
            rows = lax.dot_general(
                lhs[...], table_ref[0, first:last, :], (((1,), (1,)), ((), ())),
                preferred_element_type=F32,
            )
            k = lax.broadcasted_iota(jnp.int32, (1, last - first), 1) + first
            field[:, first:last] = jnp.where(k < length, rows, 0.0).astype(BF16)

        @pl.when(first >= length)
        def _():
            field[:, first:last] = jnp.zeros((280, last - first), BF16)

    for c in range(69):
        out_ref[c, 0] = field[4 * c : 4 * c + 4, :]


def per_device(grid, cycle_ids, cycle_len, wave_ids, legendre, target, step_w, chan_w):
    seg = grid.shape[4]
    lat_index = lax.axis_index(LAT)
    my_cycles = lax.dynamic_slice_in_dim(cycle_ids, lat_index * 10, 10)
    lengths = jnp.take(cycle_len, my_cycles)
    flengths = lengths.astype(F32)
    waves = wave_ids.reshape(N_LAT, 5)
    cols = jnp.broadcast_to(waves.T[:, None, :], (5, 2, N_LAT)).reshape(1, 640).astype(F32)
    quarter = jnp.broadcast_to(
        jnp.asarray([0.0, 0.25], F32)[None, :, None], (5, 2, N_LAT)
    ).reshape(1, 640)
    grid_t = jnp.transpose(grid[0], (1, 2, 0, 3))
    smem = pl.BlockSpec(memory_space=pltpu.SMEM)
    whole = lambda *shape: pl.BlockSpec(shape, lambda i: (0,) * len(shape))
    params = pltpu.CompilerParams(vmem_limit_bytes=60 * 2**20)
    blocks = jax.ShapeDtypeStruct((N_LAT, ROWS, 128), BF16)
    fourier, tables = pl.pallas_call(
        forward_kernel,
        grid=(10,),
        in_specs=[
            smem, smem, smem,
            pl.BlockSpec((69, 1, 4, seg), lambda i: (0, i, 0, 0)),
            whole(1, 640), whole(1, 640),
        ],
        out_specs=[
            whole(N_LAT, ROWS, 128),
            pl.BlockSpec((1, seg, 640), lambda i: (i, 0, 0)),
        ],
        out_shape=[blocks, jax.ShapeDtypeStruct((10, seg, 640), BF16)],
        scratch_shapes=[
            pltpu.VMEM((48, 640), F32), pltpu.VMEM((48, 640), F32),
            pltpu.VMEM((LO, 640), F32), pltpu.VMEM((LO, 640), F32),
            pltpu.VMEM((280, seg), BF16), pltpu.VMEM((280, 640), F32),
            pltpu.VMEM((N_LAT * ROWS, 128), F32),
        ],
        compiler_params=params,
        name="forward",
    )(lengths, 1.0 / flengths, lax.rsqrt(flengths), grid_t, cols, quarter)
    fourier = lax.all_to_all(fourier, LAT, split_axis=0, concat_axis=0, tiled=True)
    ids = cycle_ids.reshape(N_LAT, 10).T.reshape(1, 640)
    leg, leg_t = pl.pallas_call(
        order_kernel,
        grid=(5,),
        in_specs=[whole(1, 640), pl.BlockSpec((1, 320, 640), lambda i: (i, 0, 0))],
        out_specs=[
            pl.BlockSpec((1, 320, 640), lambda i: (i, 0, 0)),
            pl.BlockSpec((1, 640, 320), lambda i: (i, 0, 0)),
        ],
        out_shape=[
            jax.ShapeDtypeStruct((5, 320, 640), BF16),
            jax.ShapeDtypeStruct((5, 640, 320), BF16),
        ],
        scratch_shapes=[pltpu.VMEM((640, 640), BF16)],
        compiler_params=params,
        cost_estimate=pl.CostEstimate(flops=5 * 10**9, bytes_accessed=10**7, transcendentals=0),
        name="order",
    )(ids, legendre)
    my_waves = lax.dynamic_slice_in_dim(wave_ids, lat_index * 5, 5)
    target_t = jnp.transpose(target[0], (3, 2, 1, 0, 4)).reshape(5, 2, 276, 320)
    target_t = jnp.pad(target_t, ((0, 0), (0, 0), (0, 4), (0, 0)))
    weight = jnp.repeat(step_w[0] * chan_w, 4)
    weight = jnp.pad(weight, (0, 4)).reshape(280, 1)
    back, coeff, partial_loss = pl.pallas_call(
        owner_kernel,
        grid=(5,),
        in_specs=[
            smem,
            whole(N_LAT, ROWS, 128),
            pl.BlockSpec((1, 320, 640), lambda i: (i, 0, 0)),
            pl.BlockSpec((1, 640, 320), lambda i: (i, 0, 0)),
            pl.BlockSpec((1, 2, 280, 320), lambda i: (i, 0, 0, 0)),
            whole(280, 1),
        ],
        out_specs=[
            whole(N_LAT, ROWS, 128),
            pl.BlockSpec((1, 2, 280, 320), lambda i: (i, 0, 0, 0)),
            whole(8, 320),
        ],
        out_shape=[
            blocks,
            jax.ShapeDtypeStruct((5, 2, 280, 320), F32),
            jax.ShapeDtypeStruct((8, 320), F32),
        ],
        scratch_shapes=[
            pltpu.VMEM((N_LAT * ROWS, 128), F32),
            pltpu.VMEM((640, 768), BF16),
            pltpu.VMEM((2, 384, 320), BF16),
            pltpu.VMEM((128, 320), F32),
            pltpu.VMEM((2, 640, 128), F32),
        ],
        compiler_params=params,
        name="owner",
    )(my_waves, fourier, leg, leg_t, target_t, weight)
    back = lax.all_to_all(back, LAT, split_axis=0, concat_axis=0, tiled=True)
    loss = lax.psum(jnp.sum(partial_loss), LAT_FLD) / F32(STEPS * 276 * 320 * 321 // 2)
    coeff = coeff[:, :, :276, :].reshape(5, 2, 69, 4, 320)
    coeff = jnp.transpose(coeff, (3, 2, 1, 0, 4))[None]
    field = pl.pallas_call(
        adjoint_kernel,
        grid=(10,),
        in_specs=[
            smem,
            whole(N_LAT, ROWS, 128),
            pl.BlockSpec((1, seg, 640), lambda i: (i, 0, 0)),
        ],
        out_specs=pl.BlockSpec((69, 1, 4, seg), lambda i: (0, i, 0, 0)),
        out_shape=jax.ShapeDtypeStruct((69, 10, 4, seg), BF16),
        scratch_shapes=[
            pltpu.VMEM((N_LAT * ROWS, 128), F32),
            pltpu.VMEM((280, 640), BF16),
            pltpu.VMEM((280, seg), BF16),
        ],
        compiler_params=params,
        name="adjoint",
    )(lengths, back, tables)
    field = jnp.transpose(field, (2, 0, 1, 3))[None]
    return coeff, loss, field


def solution(mesh):
    finer = Mesh(
        mesh.devices.reshape(4, 4, 4, mesh.shape["fld"]), ("lat_0", "lat_1", "lat_2", "fld")
    )
    in_specs = (
        P("fld", None, None, LAT, None),
        P(),
        P(),
        P(),
        P(LAT, None, None),
        P("fld", None, None, None, LAT, None),
        P("fld"),
        P(),
    )
    out_specs = (P("fld", None, None, None, LAT, None), P(), P("fld", None, None, LAT, None))
    return jax.shard_map(
        per_device, mesh=finer, in_specs=in_specs, out_specs=out_specs, check_vma=False
    )
```
